32 devices in a mesh: dp: 8 (over y, x, core), tensor: 4 (over z).
Axes of the slice: x: 2, y: 2, z: 4, core: 2. Of those that a mesh axis runs over, the one named last changes fastest.
Arguments:
- tokens: bfloat16 [8192, 1024], P(('dp', 'tensor')), may hold values from -6 to 6
- upstream: bfloat16 [8192, 1024], P(('dp', 'tensor')), may hold values from -6 to 6
- counts: int32 [128], P('dp'), may hold values from 37 to 49, as said below
- norm_gain: float32 [1024], replicated, may hold values from 0.5 to 1.5
- norm_bias: float32 [1024], replicated, may hold values from -4 to 4
- w_qkv: bfloat16 [1024, 3072], P('dp', 'tensor'), may hold values from -0.1875 to 0.1875
- w_out: bfloat16 [1024, 1024], P('tensor', 'dp'), may hold values from -0.1875 to 0.1875
Outputs:
- grad_tokens: bfloat16 [8192, 1024], P(('dp', 'tensor'))
- grad_qkv: float32 [1024, 3072], P('dp', 'tensor')
- grad_out: float32 [1024, 1024], P('tensor', 'dp')
- grad_gain: float32 [1024], replicated
- grad_bias: float32 [1024], replicated
The draws below stay inside these ranges and needn't reach their ends.
Inputs may be any that keep to these rules, and one draw needn't show every extreme that they name: counts[i] is the number of visible tokens of image i, held in its first slots; some image has 49 in every draw.
All inputs are finite; a program needn't handle non-finite values.
Results may differ from the reference program's by a relative error of at most 0.014.
Values may be sent and summed in bfloat16 or wider, within the bound.
A program may use at most 64 MiB of HBM per device.

```python
import jax
import jax.numpy as jnp
from jax import lax

D = 1024
HEADS = 16
HEAD = 64
CAP = 64
MAXC = 49
MINC = 37
IMAGES = 128
TOKENS = 8192


def draw_counts(key, part):
    values = jax.random.randint(key, (IMAGES,), MINC, MAXC + 1, dtype=jnp.int32)
    position = jax.random.randint(jax.random.fold_in(key, 17), (), 0, IMAGES, dtype=jnp.int32)
    return values.at[position].set(MAXC)


def levels(stream_key, dims, cuts, low, high):
    factor_of = 1.0
    for dim, parts in cuts:
        draws = jax.random.uniform(jax.random.fold_in(jax.random.fold_in(stream_key, 6), dim), (parts,), jnp.float32, low / len(cuts), high / len(cuts))
        factor_of = factor_of * jnp.repeat(jnp.exp(draws), dims[dim] // parts).reshape((-1,) + (1,) * (len(dims) - 1 - dim))
    return factor_of


def noise(own_key, extent, scale, reach, cuts=(), kind=jnp.bfloat16):
    loudness = levels(own_key, extent, cuts, -0.22, 0.18) if cuts else 1.0
    values = jax.random.normal(own_key, extent, jnp.float32) * scale * loudness
    return jnp.minimum(jnp.maximum(values, -reach), reach).astype(kind)


def setup_inputs(seed: int = 0) -> dict:
    splits = jax.random.split(jax.random.key(seed), 8)
    return {
        "tokens": noise(splits[0], (TOKENS, D), 1.0, 6.0, ((0, 32),)),
        "upstream": noise(splits[1], (TOKENS, D), 1.0, 6.0, ((0, 32),)),
        "counts": draw_counts(jax.random.fold_in(splits[7], 71), 0),
        "norm_gain": jnp.clip(1.0 + 0.1 * jax.random.normal(splits[3], (D,), jnp.float32), 0.5, 1.5),
        "norm_bias": noise(splits[4], (D,), 1.0, 4.0, (), jnp.float32),
        "w_qkv": noise(splits[5], (D, 3 * D), D ** -0.5, 0.1875, ((0, 8), (1, 4))),
        "w_out": noise(splits[6], (D, D), D ** -0.5, 0.1875, ((0, 4), (1, 8))),
    }


def layer_norm(tokens, norm_gain, norm_bias):
    values = tokens.astype(jnp.float32)
    centre = lax.optimization_barrier(jnp.mean(values, axis=-1, keepdims=True))
    shifted = values - centre
    variance = lax.optimization_barrier(jnp.mean(shifted * shifted, axis=-1, keepdims=True))
    inverse_std = lax.rsqrt(variance + 1e-06)
    scaled = shifted * inverse_std
    normed = (scaled * norm_gain + norm_bias).astype(jnp.bfloat16)
    return (normed, scaled, inverse_std)

def reference(tokens, upstream, counts, norm_gain, norm_bias, w_qkv, w_out):
    total = tokens.shape[0]
    images = total // CAP
    slot_live = jnp.arange(CAP, dtype=jnp.int32)[None, :] < counts[:, None]
    live = slot_live.reshape(-1).astype(jnp.float32)
    normed, scaled, inverse_std = layer_norm(tokens, norm_gain, norm_bias)
    projected = jnp.dot(normed, w_qkv, preferred_element_type=jnp.float32).astype(jnp.bfloat16)
    projected = projected.reshape(images, CAP, HEADS, 3, HEAD)
    query_rows = projected[:, :, :, 0].astype(jnp.float32)
    key_rows = projected[:, :, :, 1].astype(jnp.float32)
    value_rows = projected[:, :, :, 2].astype(jnp.float32)
    score_scale = 1.0 / HEAD ** 0.5
    scores = jnp.einsum('bqhe,bkhe->bhqk', query_rows, key_rows) * score_scale
    scores = jnp.where(slot_live[:, None, None, :], scores, -1e+30)
    probs = jax.nn.softmax(scores, axis=-1)
    probs_low = probs.astype(jnp.bfloat16).astype(jnp.float32)
    attended = jnp.einsum('bhqk,bkhe->bqhe', probs_low, value_rows).astype(jnp.bfloat16).reshape(total, D)
    masked = (upstream.astype(jnp.float32) * live[:, None]).astype(jnp.bfloat16)
    grad_out = lax.dot_general(attended, masked, (((0,), (0,)), ((), ())), preferred_element_type=jnp.float32)
    grad_att = lax.dot_general(masked, w_out, (((1,), (1,)), ((), ())), preferred_element_type=jnp.float32)
    grad_att = grad_att.astype(jnp.bfloat16).reshape(images, CAP, HEADS, HEAD).astype(jnp.float32)
    grad_probs = jnp.einsum('bqhe,bkhe->bhqk', grad_att, value_rows)
    row_delta = lax.optimization_barrier(jnp.sum(probs * grad_probs, axis=-1, keepdims=True))
    grad_scores = (probs * (grad_probs - row_delta) * score_scale).astype(jnp.bfloat16).astype(jnp.float32)
    grad_value = jnp.einsum('bhqk,bqhe->bkhe', probs_low, grad_att).astype(jnp.bfloat16)
    grad_query = jnp.einsum('bhqk,bkhe->bqhe', grad_scores, key_rows).astype(jnp.bfloat16)
    grad_key = jnp.einsum('bhqk,bqhe->bkhe', grad_scores, query_rows).astype(jnp.bfloat16)
    grad_proj = jnp.stack([grad_query, grad_key, grad_value], axis=3).reshape(total, 3 * D)
    grad_qkv = lax.dot_general(normed, grad_proj, (((0,), (0,)), ((), ())), preferred_element_type=jnp.float32)
    grad_normed = lax.dot_general(grad_proj, w_qkv, (((1,), (1,)), ((), ())), preferred_element_type=jnp.float32)
    grad_gain = lax.optimization_barrier(jnp.sum(grad_normed * scaled, axis=0))
    grad_bias = lax.optimization_barrier(jnp.sum(grad_normed, axis=0))
    grad_scaled = grad_normed * norm_gain
    grad_ln = inverse_std * (grad_scaled - lax.optimization_barrier(jnp.mean(grad_scaled, axis=-1, keepdims=True)) - scaled * lax.optimization_barrier(jnp.mean(grad_scaled * scaled, axis=-1, keepdims=True)))
    grad_tokens = (upstream.astype(jnp.float32) * live[:, None] + grad_ln).astype(jnp.bfloat16)
    return (grad_tokens, grad_qkv, grad_out, grad_gain, grad_bias)
```

```python
import functools

import jax
import jax.numpy as jnp
from jax import lax
from jax.experimental import pallas as pl
from jax.experimental.pallas import tpu as pltpu
from jax.sharding import PartitionSpec as P

HEAD = 64
CAP = 64
MAXC = 49
F32 = jnp.float32
BF16 = jnp.bfloat16


def mm(a, b):
    return lax.dot_general(a, b, (((1,), (0,)), ((), ())), preferred_element_type=F32)


def mm_nt(a, b):
    return lax.dot_general(a, b, (((1,), (1,)), ((), ())), preferred_element_type=F32)


def mm_tn(a, b):
    return lax.dot_general(a, b, (((0,), (0,)), ((), ())), preferred_element_type=F32)


def image_of(index, images):
    total = jnp.zeros_like(index)
    for i in range(1, images + 1):
        total = total + jnp.where(index >= i * MAXC, 1, 0)
    return total


def packing(rows, local_rows, images):
    row = lax.broadcasted_iota(jnp.int32, (rows, 1), 0)
    image = image_of(row, images)
    source = jnp.where(image < images, image * CAP + (row - image * MAXC), -1)
    column = lax.broadcasted_iota(jnp.int32, (rows, local_rows), 1)
    return jnp.where(column == source, 1.0, 0.0).astype(BF16)


def kernel(
    n_dp, n_t,
    counts, tokens, upstream, gain, bias, wblk,
    gt_ref, gw_ref, gb_ref,
    x_all, u_all, k_all, w_all, xhat, rstd_s, gp_all, att_all, gn_send, gn_recv,
    g_send, g_recv, z_send, z_up, z_down, acc_s, fin, a_buf, b_buf, c_buf,
    xs, xr, us, ur, ks, kr, w1s, w1r, wus, wds, wzr, wgs, wgr,
    gns, gnr, ggs, ggr, gzs, gur, gdr, fs, fr, a_s, a_r, b_s, b_r, c_s, c_r,
):
    n_g = n_dp // n_t
    n_x = n_t // 2
    dp = lax.axis_index("dp")
    z = lax.axis_index("tensor")
    g = dp // n_t
    hh = dp % n_t
    xx = hh // 2
    core = hh % 2
    local_rows, width = tokens.shape
    images = local_rows // CAP
    rows = xhat.shape[0]
    wrows, cols = wblk.shape
    hw = cols // 4
    heads = hw // HEAD

    def rc(src, dst, ss, rs, dev):
        return pltpu.make_async_remote_copy(
            src_ref=src, dst_ref=dst, send_sem=ss, recv_sem=rs, device_id=dev,
            device_id_type=pl.DeviceIdType.MESH,
        )

    def member(h):
        return (g * n_t + h, z)

    def wrow(gi, b):
        return pl.ds(pl.multiple_of((gi * n_t + b) * wrows, wrows), wrows)

    def arow(j):
        return pl.ds(pl.multiple_of(j * rows, 16), rows)

    barrier = pltpu.get_barrier_semaphore()
    for i in range(1, n_t):
        pl.semaphore_signal(barrier, inc=1, device_id=member((hh + i) % n_t), device_id_type=pl.DeviceIdType.MESH)
        pl.semaphore_signal(barrier, inc=1, device_id=(dp, (z + i) % n_t), device_id_type=pl.DeviceIdType.MESH)
    for i in range(1, n_g):
        pl.semaphore_signal(
            barrier, inc=1, device_id=(((g + i) % n_g) * n_t + hh, z), device_id_type=pl.DeviceIdType.MESH
        )
    pl.semaphore_wait(barrier, 2 * (n_t - 1) + n_g - 1)

    is_root = z == hh
    go_up = jnp.logical_and(z >= hh, z < n_t - 1)
    go_down = jnp.logical_and(z <= hh, z > 0)
    next_up = (dp, (z + 1) % n_t)
    next_down = (dp, (z + n_t - 1) % n_t)

    def w_first():
        return rc(wblk, w_all.at[wrow(g, hh)], w1s, w1r.at[hh], member(z))

    @pl.when(jnp.logical_not(is_root))
    def _():
        w_first().start()

    @pl.when(is_root)
    def _():
        w_all[wrow(g, hh), :] = wblk[...]

    select = packing(rows, local_rows, images)
    row = lax.broadcasted_iota(jnp.int32, (rows, 1), 0)
    image = image_of(row, images)
    slot = row - image * MAXC
    count_of = jnp.zeros((rows, 1), jnp.int32)
    key = lax.broadcasted_iota(jnp.int32, (8, k_all.shape[2]), 1)
    key_image = image_of(key, images)
    key_slot = key - key_image * MAXC
    key_count = jnp.zeros(key.shape, jnp.int32)
    for i in range(images):
        count = counts[z * images + i]
        count_of = jnp.where(image == i, count, count_of)
        key_count = jnp.where(key_image == i, count, key_count)
    k_all[hh] = jnp.where(key_slot < key_count, key_image.astype(F32), -1.0)
    live = jnp.where(slot < count_of, 1.0, 0.0)

    partner = hh + 1 - 2 * core

    def k_copy(i):
        return rc(k_all.at[hh], k_all.at[hh], ks.at[i - 1], kr.at[hh], member((hh + i) % n_t))

    def own_copy(buf, ss, rs, i):
        dest = partner if i == 0 else ((xx + i) % n_x) * 2 + core
        return rc(buf.at[arow(hh)], buf.at[arow(hh)], ss.at[i], rs.at[hh], member(dest))

    def relay_copy(buf, ss, rs, i):
        j = ((xx + i) % n_x) * 2 + core
        return rc(buf.at[arow(j)], buf.at[arow(j)], ss.at[n_x + i - 1], rs.at[j], member(partner))

    def arrival(buf, ss, rs, j):
        return rc(buf.at[arow(j)], buf.at[arow(j)], ss.at[0], rs.at[j], member(partner))

    values = mm(select, tokens[...])
    centre = jnp.mean(values, axis=-1, keepdims=True)
    shifted = values - centre
    inverse = lax.rsqrt(jnp.mean(shifted * shifted, axis=-1, keepdims=True) + 1e-06)
    scaled = shifted * inverse
    xhat[...] = scaled
    rstd_s[...] = inverse
    x_all[arow(hh), :] = (scaled * gain[...] + bias[...]).astype(BF16)
    u_all[arow(hh), :] = (mm(select, upstream[...]) * live).astype(BF16)
    for i in range(1, n_t):
        k_copy(i).start()
    for i in range(n_x):
        own_copy(x_all, xs, xr, i).start()
    for i in range(n_x):
        own_copy(u_all, us, ur, i).start()

    def w_up(b):
        return rc(w_all.at[wrow(g, b)], w_all.at[wrow(g, b)], wus.at[b], wzr.at[b], next_up)

    def w_down(b):
        return rc(w_all.at[wrow(g, b)], w_all.at[wrow(g, b)], wds.at[b], wzr.at[b], next_down)

    def w_group(b, i):
        k = (i - 1) * n_t + b
        return rc(
            w_all.at[wrow(g, b)], w_all.at[wrow(g, b)], wgs.at[k], wgr.at[k],
            (((g + i) % n_g) * n_t + hh, z),
        )

    def w_group_arrival(b, i):
        k = (i - 1) * n_t + b
        src = w_all.at[wrow((g + n_g - i) % n_g, b)]
        return rc(src, src, wgs.at[k], wgr.at[k], (((g + i) % n_g) * n_t + hh, z))

    for b in range(n_t):
        block = w_all.at[wrow(g, b)]

        @pl.when(jnp.logical_and(is_root, hh != b))
        def _():
            rc(block, block, w1s, w1r.at[b], member(partner)).wait_recv()

        @pl.when(jnp.logical_not(is_root))
        def _():
            rc(block, block, wus.at[b], wzr.at[b], next_up).wait_recv()

        @pl.when(go_up)
        def _():
            w_up(b).start()

        @pl.when(go_down)
        def _():
            w_down(b).start()

        for i in range(1, n_g):
            w_group(b, i).start()
        if b == 0:
            for buf, ss, rs in ((x_all, xs, xr),):
                for i in range(1, n_x):
                    arrival(buf, ss, rs, ((xx + i) % n_x) * 2 + core).wait_recv()
                    relay_copy(buf, ss, rs, i).start()

    for i in range(1, n_x):
        arrival(u_all, us, ur, ((xx + i) % n_x) * 2 + core).wait_recv()
        relay_copy(u_all, us, ur, i).start()
    for buf, ss, rs in ((x_all, xs, xr), (u_all, us, ur)):
        arrival(buf, ss, rs, partner).wait_recv()
        for i in range(1, n_x):
            arrival(buf, ss, rs, ((xx + i) % n_x) * 2 + 1 - core).wait_recv()
    for i in range(1, n_t):
        j = (hh + n_t - i) % n_t
        rc(k_all.at[j], k_all.at[j], ks.at[i - 1], kr.at[j], member(partner)).wait_recv()
    for i in range(1, n_g):
        for b in range(n_t):
            w_group_arrival(b, i).wait_recv()

    score_scale = 1.0 / HEAD**0.5
    lane = lax.broadcasted_iota(jnp.int32, (1, hw), 1)

    def gn_copy(j, i):
        return rc(gn_send.at[arow(j)], gn_recv.at[arow(hh)], gns.at[i], gnr.at[hh], member(j))

    def attend(i, carry):
        j = (hh + 1 + i) % n_t
        own = arow(j)
        projected = mm(x_all[own, :], w_all[:, : 3 * hw]).astype(BF16)
        g_att = mm(u_all[own, :], w_all[:, 3 * hw :]).astype(BF16)
        query, keys, value = projected[:, :hw], projected[:, hw : 2 * hw], projected[:, 2 * hw :]
        q_image = image_of(lax.broadcasted_iota(jnp.int32, (rows, 1), 0), images).astype(F32)
        allowed = q_image == k_all[j][0:1, :rows]
        zero = jnp.zeros((rows, hw), F32)
        att, dq, dk, dv = zero, zero, zero, zero
        for h in range(heads):
            here = jnp.where(jnp.logical_and(lane >= h * HEAD, lane < (h + 1) * HEAD), 1.0, 0.0).astype(BF16)
            qh = query * here
            gh = g_att * here
            scores = jnp.where(allowed, mm_nt(qh, keys) * score_scale, -1e30)
            top = jnp.max(scores, axis=-1, keepdims=True)
            weight = jnp.exp(scores - top)
            probs = weight * (1.0 / jnp.sum(weight, axis=-1, keepdims=True))
            probs_low = probs.astype(BF16)
            att += mm(probs_low, value * here)
            g_probs = mm_nt(gh, value)
            delta = jnp.sum(probs * g_probs, axis=-1, keepdims=True)
            g_scores = (probs * (g_probs - delta) * score_scale).astype(BF16)
            dv += mm_tn(probs_low, gh)
            dq += mm(g_scores, keys * here)
            dk += mm_tn(g_scores, qh)
        att_all[own, :] = att.astype(BF16)
        gp_all[own, :hw] = dq.astype(BF16)
        gp_all[own, hw : 2 * hw] = dk.astype(BF16)
        gp_all[own, 2 * hw :] = dv.astype(BF16)
        part = mm_nt(gp_all[own, :], w_all[:, : 3 * hw]).astype(BF16)

        @pl.when(i < n_t - 1)
        def _():
            gn_send[own, :] = part
            gn_copy(j, i).start()

        @pl.when(i == n_t - 1)
        def _():
            gn_recv[arow(hh), :] = part

        return carry

    lax.fori_loop(0, n_t, attend, 0)

    half = width // n_g
    chunk = min(256, half)

    def g_copy(b, i):
        k = (i - 1) * n_t + b
        other = (g + i) % n_g
        return rc(
            g_send.at[wrow(other, b)], g_recv.at[pl.ds(k * wrows, wrows)], ggs.at[k], ggr.at[k],
            (other * n_t + hh, z),
        )

    for i in list(range(1, n_g)) + [0]:
        other = (g + i) % n_g
        for part in range(half // chunk):
            span = pl.ds(pl.multiple_of(other * half + part * chunk, 128), chunk)
            g_send[span, : 3 * hw] = mm_tn(x_all[:, span], gp_all[...]).astype(BF16)
            g_send[span, 3 * hw :] = mm_tn(u_all[:, span], att_all[...]).astype(BF16)
            if i:
                for b in range(n_t):
                    if (b + 1) * wrows <= (part + 1) * chunk and (b + 1) * wrows > part * chunk:
                        g_copy(b, i).start()

    for i in range(1, n_t):
        j = (hh + n_t - i) % n_t
        rc(gn_recv.at[arow(j)], gn_recv.at[arow(j)], gns.at[0], gnr.at[j], member(partner)).wait_recv()
    g_normed = gn_recv[pl.ds(0, rows), :].astype(F32)
    for j in range(1, n_t):
        g_normed = g_normed + gn_recv[pl.ds(j * rows, rows), :].astype(F32)
    scaled = xhat[...]
    a_buf[hh, 0:1, :] = jnp.sum(g_normed * scaled, axis=0, keepdims=True)
    a_buf[hh, 1:2, :] = jnp.sum(g_normed, axis=0, keepdims=True)

    def a_copy(i):
        return rc(a_buf.at[hh], a_buf.at[hh], a_s.at[i - 1], a_r.at[hh], member((hh + i) % n_t))

    def b_copy(i):
        return rc(b_buf.at[z], b_buf.at[z], b_s.at[i - 1], b_r.at[z], (dp, (z + i) % n_t))

    def c_copy(i):
        return rc(c_buf.at[g], c_buf.at[g], c_s.at[i - 1], c_r.at[g], (((g + i) % n_g) * n_t + hh, z))

    for i in range(1, n_t):
        a_copy(i).start()
    g_scaled = g_normed * gain[...]
    g_ln = rstd_s[...] * (
        g_scaled
        - jnp.mean(g_scaled, axis=-1, keepdims=True)
        - scaled * jnp.mean(g_scaled * scaled, axis=-1, keepdims=True)
    )
    packed = (u_all[arow(hh), :].astype(F32) + g_ln).astype(BF16)
    gt_ref[...] = mm_tn(packing(rows, local_rows, images), packed).astype(BF16)
    for i in range(1, n_t):
        j = (hh + n_t - i) % n_t
        rc(a_buf.at[j], a_buf.at[j], a_s.at[0], a_r.at[j], member(partner)).wait_recv()
    total = a_buf[0]
    for j in range(1, n_t):
        total = total + a_buf[j]
    b_buf[z] = total
    for i in range(1, n_t):
        b_copy(i).start()

    def zrow(b):
        return pl.ds(b * wrows, wrows)

    def z_up_copy(b):
        return rc(z_send.at[zrow(b)], z_down.at[zrow(b)], gzs.at[b], gdr.at[b], next_up)

    def z_down_copy(b):
        return rc(z_send.at[zrow(b)], z_up.at[zrow(b)], gzs.at[b], gur.at[b], next_down)

    def final_copy(b):
        return rc(z_send.at[zrow(b)], fin, fs.at[b], fr, member(b))

    for b in range(n_t):
        total = g_send[wrow(g, b), :].astype(F32)
        for i in range(1, n_g):
            k = (i - 1) * n_t + b
            g_copy(b, i).wait_recv()
            total = total + g_recv[pl.ds(k * wrows, wrows), :].astype(F32)
        acc_s[...] = total

        @pl.when(go_up)
        def _():
            rc(z_up.at[zrow(b)], z_up.at[zrow(b)], gzs.at[b], gur.at[b], next_up).wait_recv()
            acc_s[...] += z_up[zrow(b), :].astype(F32)

        @pl.when(go_down)
        def _():
            rc(z_down.at[zrow(b)], z_down.at[zrow(b)], gzs.at[b], gdr.at[b], next_down).wait_recv()
            acc_s[...] += z_down[zrow(b), :].astype(F32)

        z_send[zrow(b), :] = acc_s[...].astype(BF16)

        @pl.when(z > hh)
        def _():
            z_down_copy(b).start()

        @pl.when(z < hh)
        def _():
            z_up_copy(b).start()

        @pl.when(jnp.logical_and(is_root, hh != b))
        def _():
            final_copy(b).start()

        @pl.when(jnp.logical_and(is_root, hh == b))
        def _():
            gw_ref[...] = acc_s[...]

        if b == 0:
            for i in range(1, n_t):
                j = (z + n_t - i) % n_t
                rc(b_buf.at[j], b_buf.at[j], b_s.at[0], b_r.at[j], next_up).wait_recv()
            total = b_buf[0]
            for j in range(1, n_t):
                total = total + b_buf[j]
            c_buf[g] = total
            for i in range(1, n_g):
                c_copy(i).start()

    for i in range(1, n_g):
        j = (g + n_g - i) % n_g
        rc(c_buf.at[j], c_buf.at[j], c_s.at[0], c_r.at[j], (((g + i) % n_g) * n_t + hh, z)).wait_recv()
    total = c_buf[0]
    for j in range(1, n_g):
        total = total + c_buf[j]
    gb_ref[...] = total

    @pl.when(jnp.logical_not(is_root))
    def _():
        rc(fin, fin, fs.at[0], fr, member(partner)).wait_recv()
        gw_ref[...] = fin[...].astype(F32)

    @pl.when(jnp.logical_not(is_root))
    def _():
        w_first().wait_send()

    for i in range(1, n_t):
        k_copy(i).wait_send()
        a_copy(i).wait_send()
        b_copy(i).wait_send()
        gn_copy((hh + i) % n_t, i - 1).wait_send()
    for buf, ss, rs in ((x_all, xs, xr), (u_all, us, ur)):
        for i in range(n_x):
            own_copy(buf, ss, rs, i).wait_send()
        for i in range(1, n_x):
            relay_copy(buf, ss, rs, i).wait_send()
    for b in range(n_t):

        @pl.when(go_up)
        def _():
            w_up(b).wait_send()

        @pl.when(go_down)
        def _():
            w_down(b).wait_send()

        for i in range(1, n_g):
            w_group(b, i).wait_send()
            g_copy(b, i).wait_send()

        @pl.when(jnp.logical_not(is_root))
        def _():
            z_up_copy(b).wait_send()

        @pl.when(jnp.logical_and(is_root, hh != b))
        def _():
            final_copy(b).wait_send()

    for i in range(1, n_g):
        c_copy(i).wait_send()


def on_device(n_dp, n_t, tokens, upstream, counts, norm_gain, norm_bias, w_qkv, w_out):
    local_rows, width = tokens.shape
    n_g = n_dp // n_t
    n_x = n_t // 2
    wrows = w_qkv.shape[0]
    hw = w_out.shape[0]
    heads = hw // HEAD
    cols = 4 * hw
    rows = -(-(local_rows // CAP * MAXC) // 16) * 16
    lanes = -(-rows // 128) * 128
    by_kind = w_qkv.reshape(wrows, heads, 3, HEAD).transpose(0, 2, 1, 3).reshape(wrows, 3 * hw)
    wblk = jnp.concatenate([by_kind, w_out.T], axis=1)
    vmem = pl.BlockSpec(memory_space=pltpu.VMEM)
    dma = pltpu.SemaphoreType.DMA
    others = max(n_g - 1, 1)
    grad_tokens, grad_w, grad_gb = pl.pallas_call(
        functools.partial(kernel, n_dp, n_t),
        out_shape=(
            jax.ShapeDtypeStruct((local_rows, width), BF16),
            jax.ShapeDtypeStruct((wrows, cols), F32),
            jax.ShapeDtypeStruct((2, width), F32),
        ),
        in_specs=[pl.BlockSpec(memory_space=pltpu.SMEM)] + [vmem] * 5,
        out_specs=(vmem, vmem, vmem),
        scratch_shapes=[
            pltpu.VMEM((n_t * rows, width), BF16),
            pltpu.VMEM((n_t * rows, width), BF16),
            pltpu.VMEM((n_t, 8, lanes), F32),
            pltpu.VMEM((width, cols), BF16),
            pltpu.VMEM((rows, width), F32),
            pltpu.VMEM((rows, 1), F32),
            pltpu.VMEM((n_t * rows, 3 * hw), BF16),
            pltpu.VMEM((n_t * rows, hw), BF16),
            pltpu.VMEM((n_t * rows, width), BF16),
            pltpu.VMEM((n_t * rows, width), BF16),
            pltpu.VMEM((width, cols), BF16),
            pltpu.VMEM((others * n_t * wrows, cols), BF16),
            pltpu.VMEM((n_t * wrows, cols), BF16),
            pltpu.VMEM((n_t * wrows, cols), BF16),
            pltpu.VMEM((n_t * wrows, cols), BF16),
            pltpu.VMEM((wrows, cols), F32),
            pltpu.VMEM((wrows, cols), BF16),
            pltpu.VMEM((n_t, 2, width), F32),
            pltpu.VMEM((n_t, 2, width), F32),
            pltpu.VMEM((n_g, 2, width), F32),
            dma((2 * n_x,)), dma((n_t,)), dma((2 * n_x,)), dma((n_t,)),
            dma((n_t,)), dma((n_t,)),
            dma, dma((n_t,)), dma((n_t,)), dma((n_t,)), dma((n_t,)),
            dma((others * n_t,)), dma((others * n_t,)),
            dma((n_t,)), dma((n_t,)),
            dma((others * n_t,)), dma((others * n_t,)),
            dma((n_t,)), dma((n_t,)), dma((n_t,)), dma((n_t,)), dma,
            dma((n_t,)), dma((n_t,)), dma((n_t,)), dma((n_t,)), dma((n_t,)), dma((n_t,)),
        ],
        compiler_params=pltpu.CompilerParams(
            collective_id=0, has_side_effects=True, vmem_limit_bytes=56 << 20
        ),
    )(counts, tokens, upstream, norm_gain.reshape(1, -1), norm_bias.reshape(1, -1), wblk)
    grad_qkv = (
        grad_w[:, : 3 * hw].reshape(wrows, 3, heads, HEAD).transpose(0, 2, 1, 3).reshape(wrows, 3 * hw)
    )
    return (grad_tokens, grad_qkv, grad_w[:, 3 * hw :].T, grad_gb[0], grad_gb[1])


def solution(mesh):
    return jax.shard_map(
        functools.partial(on_device, mesh.shape["dp"], mesh.shape["tensor"]),
        mesh=mesh,
        in_specs=(
            P(("dp", "tensor"), None),
            P(("dp", "tensor"), None),
            P("dp"),
            P(),
            P(),
            P("dp", "tensor"),
            P("tensor", "dp"),
        ),
        out_specs=(P(("dp", "tensor"), None), P("dp", "tensor"), P("tensor", "dp"), P(), P()),
        check_vma=False,
    )
```

```python
import functools

import jax
import jax.numpy as jnp
from jax import lax
from jax.experimental import pallas as pl
from jax.experimental.pallas import tpu as pltpu
from jax.sharding import PartitionSpec as P

HEAD = 64
CAP = 64
SPLIT = 4
MAXC = 49
F32 = jnp.float32
BF16 = jnp.bfloat16


def mm(a, b):
    return lax.dot_general(a, b, (((1,), (0,)), ((), ())), preferred_element_type=F32)


def mm_nt(a, b):
    return lax.dot_general(a, b, (((1,), (1,)), ((), ())), preferred_element_type=F32)


def mm_tn(a, b):
    return lax.dot_general(a, b, (((0,), (0,)), ((), ())), preferred_element_type=F32)


def image_of(index, images):
    total = jnp.zeros_like(index)
    for i in range(1, images + 1):
        total = total + jnp.where(index >= i * MAXC, 1, 0)
    return total


def packing(rows, local_rows, images):
    row = lax.broadcasted_iota(jnp.int32, (rows, 1), 0)
    image = image_of(row, images)
    source = jnp.where(image < images, image * CAP + (row - image * MAXC), -1)
    column = lax.broadcasted_iota(jnp.int32, (rows, local_rows), 1)
    return jnp.where(column == source, 1.0, 0.0).astype(BF16)


def kernel(
    n_dp, n_t,
    counts, tokens, upstream, gain, bias, wblk,
    gt_ref, gw_ref, gb_ref,
    x_all, u_all, k_all, w_all, xhat, rstd_s, gp_all, att_all, gn_send, gn_recv,
    g_send, g_recv, z_send, z_up, z_down, acc_s, fin, a_buf, b_buf, c_buf,
    xs, xr, us, ur, ks, kr, w1s, w1r, wus, wds, wzr, wgs, wgr,
    gns, gnr, ggs, ggr, gzs, gur, gdr, fs, fr, a_s, a_r, b_s, b_r, c_s, c_r,
):
    n_g = n_dp // n_t
    n_x = n_t // 2
    dp = lax.axis_index("dp")
    z = lax.axis_index("tensor")
    g = dp // n_t
    hh = dp % n_t
    xx = hh // 2
    core = hh % 2
    local_rows, width = tokens.shape
    images = local_rows // CAP
    rows = xhat.shape[0]
    wrows, cols = wblk.shape
    hw = cols // 4
    heads = hw // HEAD

    def rc(src, dst, ss, rs, dev):
        return pltpu.make_async_remote_copy(
            src_ref=src, dst_ref=dst, send_sem=ss, recv_sem=rs, device_id=dev,
            device_id_type=pl.DeviceIdType.MESH,
        )

    def member(h):
        return (g * n_t + h, z)

    prow = wrows // SPLIT
    pieces = n_t * SPLIT

    def wrow(gi, p):
        return pl.ds(pl.multiple_of((gi * pieces + p) * prow, prow), prow)

    def near(k):
        return ((xx + k // (2 * SPLIT)) % n_x) * 2 + (core + (k // SPLIT) % 2) % 2

    order = [(near(k), near(k) * SPLIT + k % SPLIT, k) for k in range(pieces)]

    def arow(j):
        return pl.ds(pl.multiple_of(j * rows, 16), rows)

    barrier = pltpu.get_barrier_semaphore()
    for i in range(1, n_t):
        pl.semaphore_signal(barrier, inc=1, device_id=member((hh + i) % n_t), device_id_type=pl.DeviceIdType.MESH)
        pl.semaphore_signal(barrier, inc=1, device_id=(dp, (z + i) % n_t), device_id_type=pl.DeviceIdType.MESH)
    for i in range(1, n_g):
        pl.semaphore_signal(
            barrier, inc=1, device_id=(((g + i) % n_g) * n_t + hh, z), device_id_type=pl.DeviceIdType.MESH
        )
    pl.semaphore_wait(barrier, 2 * (n_t - 1) + n_g - 1)

    is_root = z == hh
    go_up = jnp.logical_and(z >= hh, z < n_t - 1)
    go_down = jnp.logical_and(z <= hh, z > 0)
    next_up = (dp, (z + 1) % n_t)
    next_down = (dp, (z + n_t - 1) % n_t)

    def w_first(s):
        p = hh * SPLIT + s
        return rc(wblk.at[pl.ds(s * prow, prow)], w_all.at[wrow(g, p)], w1s.at[s], w1r.at[p], member(z))

    for s in range(SPLIT):

        @pl.when(jnp.logical_not(is_root))
        def _():
            w_first(s).start()

        @pl.when(is_root)
        def _():
            w_all[wrow(g, hh * SPLIT + s), :] = wblk[pl.ds(s * prow, prow), :]

    select = packing(rows, local_rows, images)
    row = lax.broadcasted_iota(jnp.int32, (rows, 1), 0)
    image = image_of(row, images)
    slot = row - image * MAXC
    count_of = jnp.zeros((rows, 1), jnp.int32)
    key = lax.broadcasted_iota(jnp.int32, (8, k_all.shape[2]), 1)
    key_image = image_of(key, images)
    key_slot = key - key_image * MAXC
    key_count = jnp.zeros(key.shape, jnp.int32)
    for i in range(images):
        count = counts[z * images + i]
        count_of = jnp.where(image == i, count, count_of)
        key_count = jnp.where(key_image == i, count, key_count)
    k_all[hh] = jnp.where(key_slot < key_count, key_image.astype(F32), -1.0)
    live = jnp.where(slot < count_of, 1.0, 0.0)

    partner = hh + 1 - 2 * core

    def k_copy(i):
        return rc(k_all.at[hh], k_all.at[hh], ks.at[i - 1], kr.at[hh], member((hh + i) % n_t))

    def own_copy(buf, ss, rs, i):
        dest = partner if i == 0 else ((xx + i) % n_x) * 2 + core
        return rc(buf.at[arow(hh)], buf.at[arow(hh)], ss.at[i], rs.at[hh], member(dest))

    def relay_copy(buf, ss, rs, i):
        j = ((xx + i) % n_x) * 2 + core
        return rc(buf.at[arow(j)], buf.at[arow(j)], ss.at[n_x + i - 1], rs.at[j], member(partner))

    def arrival(buf, ss, rs, j):
        return rc(buf.at[arow(j)], buf.at[arow(j)], ss.at[0], rs.at[j], member(partner))

    values = mm(select, tokens[...])
    centre = jnp.mean(values, axis=-1, keepdims=True)
    shifted = values - centre
    inverse = lax.rsqrt(jnp.mean(shifted * shifted, axis=-1, keepdims=True) + 1e-06)
    scaled = shifted * inverse
    xhat[...] = scaled
    rstd_s[...] = inverse
    x_all[arow(hh), :] = (scaled * gain[...] + bias[...]).astype(BF16)
    u_all[arow(hh), :] = (mm(select, upstream[...]) * live).astype(BF16)
    for i in range(1, n_t):
        k_copy(i).start()
    for i in range(n_x):
        own_copy(x_all, xs, xr, i).start()
    for i in range(n_x):
        own_copy(u_all, us, ur, i).start()

    def w_up(b):
        return rc(w_all.at[wrow(g, b)], w_all.at[wrow(g, b)], wus.at[b], wzr.at[b], next_up)

    def w_down(b):
        return rc(w_all.at[wrow(g, b)], w_all.at[wrow(g, b)], wds.at[b], wzr.at[b], next_down)

    def w_group(b, i):
        k = (i - 1) * pieces + b
        return rc(
            w_all.at[wrow(g, b)], w_all.at[wrow(g, b)], wgs.at[k], wgr.at[k],
            (((g + i) % n_g) * n_t + hh, z),
        )

    def w_group_arrival(b, i):
        k = (i - 1) * pieces + b
        src = w_all.at[wrow((g + n_g - i) % n_g, b)]
        return rc(src, src, wgs.at[k], wgr.at[k], (((g + i) % n_g) * n_t + hh, z))

    for b, p, k in order:
        block = w_all.at[wrow(g, p)]

        @pl.when(jnp.logical_and(is_root, hh != b))
        def _():
            rc(block, block, w1s.at[0], w1r.at[p], member(partner)).wait_recv()

        @pl.when(jnp.logical_not(is_root))
        def _():
            rc(block, block, wus.at[p], wzr.at[p], next_up).wait_recv()

        @pl.when(go_up)
        def _():
            w_up(p).start()

        @pl.when(go_down)
        def _():
            w_down(p).start()

        for i in range(1, n_g):
            w_group(p, i).start()
        for buf, ss, rs, when in ((x_all, xs, xr, pieces // 2 + 1), (u_all, us, ur, pieces - 1)):
            if k == when:
                for i in range(1, n_x):
                    arrival(buf, ss, rs, ((xx + i) % n_x) * 2 + core).wait_recv()
                    relay_copy(buf, ss, rs, i).start()

    for buf, ss, rs in ((x_all, xs, xr), (u_all, us, ur)):
        arrival(buf, ss, rs, partner).wait_recv()
        for i in range(1, n_x):
            arrival(buf, ss, rs, ((xx + i) % n_x) * 2 + 1 - core).wait_recv()
    for i in range(1, n_t):
        j = (hh + n_t - i) % n_t
        rc(k_all.at[j], k_all.at[j], ks.at[i - 1], kr.at[j], member(partner)).wait_recv()
    for i in range(1, n_g):
        for b, p, k in order:
            w_group_arrival(p, i).wait_recv()

    score_scale = 1.0 / HEAD**0.5
    lane = lax.broadcasted_iota(jnp.int32, (1, hw), 1)

    def gn_copy(j, i):
        return rc(gn_send.at[arow(j)], gn_recv.at[arow(hh)], gns.at[i], gnr.at[hh], member(j))

    def attend(i, carry):
        j = (hh + 1 + i) % n_t
        own = arow(j)
        projected = mm(x_all[own, :], w_all[:, : 3 * hw]).astype(BF16)
        g_att = mm(u_all[own, :], w_all[:, 3 * hw :]).astype(BF16)
        query, keys, value = projected[:, :hw], projected[:, hw : 2 * hw], projected[:, 2 * hw :]
        q_image = image_of(lax.broadcasted_iota(jnp.int32, (rows, 1), 0), images).astype(F32)
        allowed = q_image == k_all[j][0:1, :rows]
        zero = jnp.zeros((rows, hw), F32)
        att, dq, dk, dv = zero, zero, zero, zero
        for h in range(heads):
            here = jnp.where(jnp.logical_and(lane >= h * HEAD, lane < (h + 1) * HEAD), 1.0, 0.0).astype(BF16)
            qh = query * here
            gh = g_att * here
            scores = jnp.where(allowed, mm_nt(qh, keys) * score_scale, -1e30)
            top = jnp.max(scores, axis=-1, keepdims=True)
            weight = jnp.exp(scores - top)
            probs = weight * (1.0 / jnp.sum(weight, axis=-1, keepdims=True))
            probs_low = probs.astype(BF16)
            att += mm(probs_low, value * here)
            g_probs = mm_nt(gh, value)
            delta = jnp.sum(probs * g_probs, axis=-1, keepdims=True)
            g_scores = (probs * (g_probs - delta) * score_scale).astype(BF16)
            dv += mm_tn(probs_low, gh)
            dq += mm(g_scores, keys * here)
            dk += mm_tn(g_scores, qh)
        att_all[own, :] = att.astype(BF16)
        gp_all[own, :hw] = dq.astype(BF16)
        gp_all[own, hw : 2 * hw] = dk.astype(BF16)
        gp_all[own, 2 * hw :] = dv.astype(BF16)
        part = mm_nt(gp_all[own, :], w_all[:, : 3 * hw]).astype(BF16)

        @pl.when(i < n_t - 1)
        def _():
            gn_send[own, :] = part
            gn_copy(j, i).start()

        @pl.when(i == n_t - 1)
        def _():
            gn_recv[arow(hh), :] = part

        return carry

    lax.fori_loop(0, n_t, attend, 0)

    half = width // n_g
    chunk = min(256, half)

    def g_copy(b, i):
        k = (i - 1) * pieces + b
        other = (g + i) % n_g
        return rc(
            g_send.at[wrow(other, b)], g_recv.at[pl.ds(pl.multiple_of(k * prow, prow), prow)], ggs.at[k], ggr.at[k],
            (other * n_t + hh, z),
        )

    for i in list(range(1, n_g)) + [0]:
        other = (g + i) % n_g
        for part in range(half // chunk):
            span = pl.ds(pl.multiple_of(other * half + part * chunk, 128), chunk)
            g_send[span, : 3 * hw] = mm_tn(x_all[:, span], gp_all[...]).astype(BF16)
            g_send[span, 3 * hw :] = mm_tn(u_all[:, span], att_all[...]).astype(BF16)
        if i:
            for b, p, k in order[::-1]:
                g_copy(p, i).start()

    def a_copy(i):
        return rc(a_buf.at[hh], a_buf.at[hh], a_s.at[i - 1], a_r.at[hh], member((hh + i) % n_t))

    def b_copy(i):
        return rc(b_buf.at[z], b_buf.at[z], b_s.at[i - 1], b_r.at[z], (dp, (z + i) % n_t))

    def c_copy(i):
        return rc(c_buf.at[g], c_buf.at[g], c_s.at[i - 1], c_r.at[g], (((g + i) % n_g) * n_t + hh, z))

    def finish_tokens():
        for i in range(1, n_t):
            j = (hh + n_t - i) % n_t
            rc(gn_recv.at[arow(j)], gn_recv.at[arow(j)], gns.at[0], gnr.at[j], member(partner)).wait_recv()
        g_normed = gn_recv[pl.ds(0, rows), :].astype(F32)
        for j in range(1, n_t):
            g_normed = g_normed + gn_recv[pl.ds(j * rows, rows), :].astype(F32)
        scaled = xhat[...]
        a_buf[hh, 0:1, :] = jnp.sum(g_normed * scaled, axis=0, keepdims=True)
        a_buf[hh, 1:2, :] = jnp.sum(g_normed, axis=0, keepdims=True)
        for i in range(1, n_t):
            a_copy(i).start()
        g_scaled = g_normed * gain[...]
        g_ln = rstd_s[...] * (
            g_scaled
            - jnp.mean(g_scaled, axis=-1, keepdims=True)
            - scaled * jnp.mean(g_scaled * scaled, axis=-1, keepdims=True)
        )
        packed = (u_all[arow(hh), :].astype(F32) + g_ln).astype(BF16)
        gt_ref[...] = mm_tn(packing(rows, local_rows, images), packed).astype(BF16)

    def reduce_first():
        for i in range(1, n_t):
            j = (hh + n_t - i) % n_t
            rc(a_buf.at[j], a_buf.at[j], a_s.at[0], a_r.at[j], member(partner)).wait_recv()
        total = a_buf[0]
        for j in range(1, n_t):
            total = total + a_buf[j]
        b_buf[z] = total
        for i in range(1, n_t):
            b_copy(i).start()

    def zrow(b):
        return pl.ds(pl.multiple_of(b * prow, prow), prow)

    def z_up_copy(b):
        return rc(z_send.at[zrow(b)], z_down.at[zrow(b)], gzs.at[b], gdr.at[b], next_up)

    def z_down_copy(b):
        return rc(z_send.at[zrow(b)], z_up.at[zrow(b)], gzs.at[b], gur.at[b], next_down)

    def final_copy(b):
        part = b % SPLIT
        return rc(
            z_send.at[zrow(b)], fin.at[zrow(part)], fs.at[b], fr.at[part], member(b // SPLIT)
        )

    for head, b, step in order[::-1]:
        total = g_send[wrow(g, b), :].astype(F32)
        for i in range(1, n_g):
            k = (i - 1) * pieces + b
            g_copy(b, i).wait_recv()
            total = total + g_recv[pl.ds(pl.multiple_of(k * prow, prow), prow), :].astype(F32)
        acc_s[...] = total

        @pl.when(go_up)
        def _():
            rc(z_up.at[zrow(b)], z_up.at[zrow(b)], gzs.at[b], gur.at[b], next_up).wait_recv()
            acc_s[...] += z_up[zrow(b), :].astype(F32)

        @pl.when(go_down)
        def _():
            rc(z_down.at[zrow(b)], z_down.at[zrow(b)], gzs.at[b], gdr.at[b], next_down).wait_recv()
            acc_s[...] += z_down[zrow(b), :].astype(F32)

        z_send[zrow(b), :] = acc_s[...].astype(BF16)

        @pl.when(z > hh)
        def _():
            z_down_copy(b).start()

        @pl.when(z < hh)
        def _():
            z_up_copy(b).start()

        @pl.when(jnp.logical_and(is_root, hh != head))
        def _():
            final_copy(b).start()

        @pl.when(jnp.logical_and(is_root, hh == head))
        def _():
            gw_ref[pl.ds((step % SPLIT) * prow, prow), :] = acc_s[...]

        if step == pieces // 2 - 1:
            finish_tokens()
        if step == min(1, pieces - 1):
            reduce_first()

    for i in range(1, n_t):
        j = (z + n_t - i) % n_t
        rc(b_buf.at[j], b_buf.at[j], b_s.at[0], b_r.at[j], next_up).wait_recv()
    total = b_buf[0]
    for j in range(1, n_t):
        total = total + b_buf[j]
    c_buf[g] = total
    for i in range(1, n_g):
        c_copy(i).start()

    for i in range(1, n_g):
        j = (g + n_g - i) % n_g
        rc(c_buf.at[j], c_buf.at[j], c_s.at[0], c_r.at[j], (((g + i) % n_g) * n_t + hh, z)).wait_recv()
    total = c_buf[0]
    for j in range(1, n_g):
        total = total + c_buf[j]
    gb_ref[...] = total

    @pl.when(jnp.logical_not(is_root))
    def _():
        for part in range(SPLIT):
            piece = fin.at[zrow(part)]
            rc(piece, piece, fs.at[part], fr.at[part], member(partner)).wait_recv()
        gw_ref[...] = fin[...].astype(F32)

    @pl.when(jnp.logical_not(is_root))
    def _():
        for s in range(SPLIT):
            w_first(s).wait_send()

    for i in range(1, n_t):
        k_copy(i).wait_send()
        a_copy(i).wait_send()
        b_copy(i).wait_send()
        gn_copy((hh + i) % n_t, i - 1).wait_send()
    for buf, ss, rs in ((x_all, xs, xr), (u_all, us, ur)):
        for i in range(n_x):
            own_copy(buf, ss, rs, i).wait_send()
        for i in range(1, n_x):
            relay_copy(buf, ss, rs, i).wait_send()
    for head, b, step in order:

        @pl.when(go_up)
        def _():
            w_up(b).wait_send()

        @pl.when(go_down)
        def _():
            w_down(b).wait_send()

        for i in range(1, n_g):
            w_group(b, i).wait_send()
            g_copy(b, i).wait_send()

        @pl.when(jnp.logical_not(is_root))
        def _():
            z_up_copy(b).wait_send()

        @pl.when(jnp.logical_and(is_root, hh != head))
        def _():
            final_copy(b).wait_send()

    for i in range(1, n_g):
        c_copy(i).wait_send()


def on_device(n_dp, n_t, tokens, upstream, counts, norm_gain, norm_bias, w_qkv, w_out):
    local_rows, width = tokens.shape
    n_g = n_dp // n_t
    n_x = n_t // 2
    wrows = w_qkv.shape[0]
    hw = w_out.shape[0]
    heads = hw // HEAD
    cols = 4 * hw
    rows = -(-(local_rows // CAP * MAXC) // 16) * 16
    lanes = -(-rows // 128) * 128
    by_kind = w_qkv.reshape(wrows, heads, 3, HEAD).transpose(0, 2, 1, 3).reshape(wrows, 3 * hw)
    wblk = jnp.concatenate([by_kind, w_out.T], axis=1)
    vmem = pl.BlockSpec(memory_space=pltpu.VMEM)
    dma = pltpu.SemaphoreType.DMA
    others = max(n_g - 1, 1)
    pieces = n_t * SPLIT
    grad_tokens, grad_w, grad_gb = pl.pallas_call(
        functools.partial(kernel, n_dp, n_t),
        out_shape=(
            jax.ShapeDtypeStruct((local_rows, width), BF16),
            jax.ShapeDtypeStruct((wrows, cols), F32),
            jax.ShapeDtypeStruct((2, width), F32),
        ),
        in_specs=[pl.BlockSpec(memory_space=pltpu.SMEM)] + [vmem] * 5,
        out_specs=(vmem, vmem, vmem),
        scratch_shapes=[
            pltpu.VMEM((n_t * rows, width), BF16),
            pltpu.VMEM((n_t * rows, width), BF16),
            pltpu.VMEM((n_t, 8, lanes), F32),
            pltpu.VMEM((width, cols), BF16),
            pltpu.VMEM((rows, width), F32),
            pltpu.VMEM((rows, 1), F32),
            pltpu.VMEM((n_t * rows, 3 * hw), BF16),
            pltpu.VMEM((n_t * rows, hw), BF16),
            pltpu.VMEM((n_t * rows, width), BF16),
            pltpu.VMEM((n_t * rows, width), BF16),
            pltpu.VMEM((width, cols), BF16),
            pltpu.VMEM((others * n_t * wrows, cols), BF16),
            pltpu.VMEM((n_t * wrows, cols), BF16),
            pltpu.VMEM((n_t * wrows, cols), BF16),
            pltpu.VMEM((n_t * wrows, cols), BF16),
            pltpu.VMEM((wrows // SPLIT, cols), F32),
            pltpu.VMEM((wrows, cols), BF16),
            pltpu.VMEM((n_t, 2, width), F32),
            pltpu.VMEM((n_t, 2, width), F32),
            pltpu.VMEM((n_g, 2, width), F32),
            dma((2 * n_x,)), dma((n_t,)), dma((2 * n_x,)), dma((n_t,)),
            dma((n_t,)), dma((n_t,)),
            dma((SPLIT,)), dma((pieces,)), dma((pieces,)), dma((pieces,)), dma((pieces,)),
            dma((others * pieces,)), dma((others * pieces,)),
            dma((n_t,)), dma((n_t,)),
            dma((others * pieces,)), dma((others * pieces,)),
            dma((pieces,)), dma((pieces,)), dma((pieces,)), dma((pieces,)), dma((SPLIT,)),
            dma((n_t,)), dma((n_t,)), dma((n_t,)), dma((n_t,)), dma((n_t,)), dma((n_t,)),
        ],
        compiler_params=pltpu.CompilerParams(
            collective_id=0, has_side_effects=True, vmem_limit_bytes=56 << 20
        ),
    )(counts, tokens, upstream, norm_gain.reshape(1, -1), norm_bias.reshape(1, -1), wblk)
    grad_qkv = (
        grad_w[:, : 3 * hw].reshape(wrows, 3, heads, HEAD).transpose(0, 2, 1, 3).reshape(wrows, 3 * hw)
    )
    return (grad_tokens, grad_qkv, grad_w[:, 3 * hw :].T, grad_gb[0], grad_gb[1])


def solution(mesh):
    return jax.shard_map(
        functools.partial(on_device, mesh.shape["dp"], mesh.shape["tensor"]),
        mesh=mesh,
        in_specs=(
            P(("dp", "tensor"), None),
            P(("dp", "tensor"), None),
            P("dp"),
            P(),
            P(),
            P("dp", "tensor"),
            P("tensor", "dp"),
        ),
        out_specs=(P(("dp", "tensor"), None), P("dp", "tensor"), P("tensor", "dp"), P(), P()),
        check_vma=False,
    )
```
